32 devices in a mesh: dp: 4 (over y, core), tensor: 2 (over x), pipe: 4 (over z).
Axes of the slice: x: 2, y: 2, z: 4, core: 2. Of those that a mesh axis runs over, the one named last changes fastest.
Arguments:
- grad_parts: float32 [4, 4, 2, 64, 8192], P('dp', 'pipe', 'tensor'), may hold values from -24 to 24
- drop_flags: int32 [4, 4, 2, 64], P('dp', 'pipe', 'tensor'), may hold values from 0 to 1, as said below
- owner_order: int32 [4], replicated, may hold values from 0 to 3, each once
- step_count: int32 [], replicated, may hold values from 1 to 11
- master: float32 [4, 2, 64, 8192], P('pipe', 'tensor', None, 'dp'), may hold values from -6 to 6
- moment_m: float32 [4, 2, 64, 8192], P('pipe', 'tensor', None, 'dp'), may hold values from -0.15625 to 0.15625
- moment_v: float32 [4, 2, 64, 8192], P('pipe', 'tensor', None, 'dp'), may hold values from 0.0001 to 0.001
Outputs:
- new_master: float32 [4, 2, 64, 8192], P('pipe', 'tensor', None, 'dp')
- new_m: float32 [4, 2, 64, 8192], P('pipe', 'tensor', None, 'dp')
- new_v: float32 [4, 2, 64, 8192], P('pipe', 'tensor', None, 'dp')
- direction: float32 [4, 2, 64, 8192], P('pipe', 'tensor', None, 'dp')
- dropped_total: int32 [], replicated
The draws below stay inside these ranges and needn't reach their ends.
Inputs may be any that keep to these rules, and one draw needn't show every extreme that they name: `drop_flags`: A row may be flagged by every replica.
All inputs are finite; a program needn't handle non-finite values.
Results may differ from the reference program's by a relative error of at most 0.0003.
Values sent between devices are 32-bit elements; how exact they have to be, the bound alone decides.
No kernel may reach another device: no remote copies, remote signals or barrier semaphores. Data moves between devices by JAX's collectives and lax.ppermute only.
A program may use at most 64 MiB of HBM per device.

```python
import math
import jax
import jax.numpy as jnp
from jax import lax

D = 8192
ROWS = 64
LAYERS = 4
SHARDS = 2
N_DP = 4


def draw_drop_flags(key, part):
    random_ones = jax.random.randint(jax.random.fold_in(key, 11), (N_DP, LAYERS, SHARDS, ROWS), 0, 4) == 0
    full_rows = jax.random.randint(jax.random.fold_in(key, 12), (LAYERS, SHARDS, ROWS), 0, 32) == 0
    forced = jax.random.randint(jax.random.fold_in(key, 13), (), 0, LAYERS * SHARDS * ROWS)
    position = jnp.arange(LAYERS * SHARDS * ROWS, dtype=jnp.int32).reshape(LAYERS, SHARDS, ROWS)
    every_replica = full_rows | (position == forced)
    return jnp.where(random_ones | every_replica[None], 1, 0).astype(jnp.int32)


def draw_grad_parts(key, part):
    block_cols = D // N_DP
    pairing = jax.random.permutation(jax.random.fold_in(key, 21), N_DP)
    column_block = jnp.arange(D, dtype=jnp.int32) // block_cols
    spiked = column_block[None, :] == pairing[:, None]
    factor = jnp.where(spiked, 4.0, 1.0).astype(jnp.float32)[:, None, None, None, :]
    noise = jax.random.normal(jax.random.fold_in(key, 22), (N_DP, LAYERS, SHARDS, ROWS, D), jnp.float32)
    own_part = jnp.clip(noise, -6.0, 6.0) * factor
    values = own_part
    return values.astype(jnp.float32)


def levels(own_key, dims, pieces, low, top_value):
    gain = 1.0
    for axis_at, shards_of in pieces:
        heights = jax.random.uniform(jax.random.fold_in(jax.random.fold_in(own_key, 6), axis_at), (shards_of,), jnp.float32, low / len(pieces), top_value / len(pieces))
        gain = gain * jnp.repeat(jnp.exp(heights), dims[axis_at] // shards_of).reshape((-1,) + (1,) * (len(dims) - 1 - axis_at))
    return gain


def gaussian(key, shape, spread, most, pieces=(), kind=jnp.bfloat16):
    array = jax.random.normal(key, shape, jnp.float32) * spread
    if len(pieces) > 0:
        array = levels(key, shape, pieces, -0.22, 0.18) * array
    return jnp.clip(array, min=-most, max=most).astype(kind)


def setup_inputs(seed: int = 0) -> dict:
    streams_of = jax.random.split(jax.random.key(seed), 8)
    return {
        "grad_parts": draw_grad_parts(jax.random.fold_in(streams_of[7], 71), 0),
        "drop_flags": draw_drop_flags(jax.random.fold_in(streams_of[7], 71), 0),
        "owner_order": jax.random.permutation(streams_of[2], N_DP).astype(jnp.int32),
        "step_count": jax.random.randint(streams_of[3], (), 1, 12).astype(jnp.int32),
        "master": gaussian(streams_of[4], (LAYERS, SHARDS, ROWS, D), 1.0, 6.0, ((0, 4), (1, 2), (3, 4)), jnp.float32),
        "moment_m": gaussian(streams_of[5], (LAYERS, SHARDS, ROWS, D), 0.01, 0.15625, ((0, 4), (1, 2), (3, 4)), jnp.float32),
        "moment_v": jnp.clip(jnp.exp(math.log(0.001) - 2.3025852 * jax.random.uniform(streams_of[6], (LAYERS, SHARDS, ROWS, D), jnp.float32) ** levels(streams_of[6], (LAYERS, SHARDS, ROWS, D), ((0, 4), (1, 2), (3, 4)), -0.2, 0.2)), 0.0001, 0.001),
    }


def reference(grad_parts, drop_flags, owner_order, step_count, master, moment_m, moment_v):
    kept = (1 - drop_flags).astype(jnp.float32)

    def accumulate(carry, pair):
        part, keep = pair
        return ((carry[0] + part * keep[..., None], carry[1] + keep), None)
    start = (jnp.zeros(grad_parts.shape[1:], jnp.float32), jnp.zeros(kept.shape[1:], jnp.float32))
    (total, count), unused = lax.scan(accumulate, start, (grad_parts, kept))
    mean_grad = total / jnp.maximum(count, 1.0)[..., None]
    shape = mean_grad.shape
    blocks = mean_grad.reshape(shape[0], shape[1], shape[2], N_DP, shape[3] // N_DP)
    grad = jnp.take(blocks, owner_order, axis=3).reshape(shape)
    entries = shape[0] * shape[1] * shape[2] * shape[3]
    rms = jnp.sqrt(jnp.sum(grad * grad) / entries)
    clip = jnp.minimum(1.0, 0.05 / (rms + 1e-06))
    scaled = clip * grad
    new_m = 0.9 * moment_m + 0.1 * scaled
    new_v = 0.999 * moment_v + 0.001 * scaled * scaled
    steps = step_count.astype(jnp.float32)
    m_hat = new_m / (1.0 - jnp.power(0.9, steps))
    v_hat = new_v / (1.0 - jnp.power(0.999, steps))
    direction = m_hat / (jnp.sqrt(v_hat) + 1e-08) + 0.1 * master
    new_master = master - 0.001 * direction
    dropped_total = jnp.sum(drop_flags).astype(jnp.int32)
    return (new_master, new_m, new_v, direction, dropped_total)
```

```python
import jax
import jax.numpy as jnp
from jax import lax
from jax.sharding import PartitionSpec as P

ALL = ("dp", "tensor", "pipe")


def body(grad_parts, drop_flags, owner_order, step_count, master, moment_m, moment_v):
    replicas = lax.axis_size("dp")
    chips = replicas // 2
    me = lax.axis_index("dp")
    chip = me // 2
    core = me % 2
    flags = drop_flags[0, 0, 0]
    kept = (1 - flags).astype(jnp.float32)
    local_grad = grad_parts[0, 0, 0]
    rows_here = local_grad.shape[0]
    width = local_grad.shape[1]
    block_cols = width // replicas

    mate_pairs = [(j, j ^ 1) for j in range(replicas)]

    def along(step):
        return [(j, (j // 2 + step) % chips * 2 + j % 2) for j in range(replicas)]

    def block_for(device):
        start = owner_order[device] * block_cols
        return lax.dynamic_slice_in_dim(local_grad, start, block_cols, 1) * kept[:, None]

    order = [(chip + step) % chips * 2 for step in range(chips)]
    for_mate = jnp.stack([block_for(base + 1 - core) for base in order])
    own = jnp.stack([block_for(base + core) for base in order])
    pair_sum = own + lax.ppermute(for_mate, "dp", mate_pairs)
    summed = pair_sum[0]
    for step in range(1, chips):
        summed = summed + lax.ppermute(pair_sum[step], "dp", along(step))

    count = kept
    for step in range(1, chips):
        count = count + lax.ppermute(kept, "dp", along(step))
    count = count + lax.ppermute(count, "dp", mate_pairs)

    grad = summed / jnp.maximum(count, 1.0)[:, None]
    lane = lax.broadcasted_iota(jnp.int32, (1, 128), 1)
    square_here = jnp.sum(grad * grad)
    dropped_here = jnp.sum(flags).astype(jnp.float32)
    row = jnp.where(lane == 0, square_here, jnp.where(lane == 1, dropped_here, 0.0))
    devices = lax.axis_size(ALL)
    rows = lax.all_to_all(jnp.broadcast_to(row[None], (devices, 1, 128)), ALL, 0, 0, tiled=True)
    totals = jnp.sum(rows, axis=0)[0]
    square_sum, dropped = totals[0], totals[1]

    entries = rows_here * width * lax.axis_size("tensor") * lax.axis_size("pipe")
    rms = jnp.sqrt(square_sum / entries)
    clip = jnp.minimum(1.0, 0.05 / (rms + 1e-06))
    scaled = clip * grad
    old_m = moment_m[0, 0]
    old_v = moment_v[0, 0]
    weights = master[0, 0]
    new_m = 0.9 * old_m + 0.1 * scaled
    new_v = 0.999 * old_v + 0.001 * scaled * scaled
    steps = step_count.astype(jnp.float32)
    m_hat = new_m / (1.0 - jnp.power(0.9, steps))
    v_hat = new_v / (1.0 - jnp.power(0.999, steps))
    direction = m_hat / (jnp.sqrt(v_hat) + 1e-08) + 0.1 * weights
    new_master = weights - 0.001 * direction
    return (
        new_master[None, None],
        new_m[None, None],
        new_v[None, None],
        direction[None, None],
        dropped.astype(jnp.int32),
    )


def solution(mesh):
    return jax.shard_map(
        body,
        mesh=mesh,
        in_specs=(
            P("dp", "pipe", "tensor", None, None),
            P("dp", "pipe", "tensor", None),
            P(),
            P(),
            P("pipe", "tensor", None, "dp"),
            P("pipe", "tensor", None, "dp"),
            P("pipe", "tensor", None, "dp"),
        ),
        out_specs=(
            P("pipe", "tensor", None, "dp"),
            P("pipe", "tensor", None, "dp"),
            P("pipe", "tensor", None, "dp"),
            P("pipe", "tensor", None, "dp"),
            P(),
        ),
        check_vma=False,
    )
```

```python
import jax
import jax.numpy as jnp
from jax import lax
from jax.experimental import pallas as pl
from jax.experimental.pallas import tpu as pltpu
from jax.sharding import PartitionSpec as P

ALL = ("dp", "tensor", "pipe")
VMEM = pltpu.MemorySpace.VMEM
SMEM = pltpu.MemorySpace.SMEM
CHUNK = 8


def in_vmem():
    return pl.BlockSpec(memory_space=VMEM)


def in_smem():
    return pl.BlockSpec(memory_space=SMEM)


def anywhere():
    return pl.BlockSpec(memory_space=pl.ANY)


def hold(x):
    return pltpu.with_memory_space_constraint(x, VMEM)


def column(row):
    n = row.shape[1]
    rows = lax.broadcasted_iota(jnp.int32, (n, n), 0)
    cols = lax.broadcasted_iota(jnp.int32, (n, n), 1)
    return jnp.sum(jnp.where(rows == cols, jnp.broadcast_to(row, (n, n)), 0.0), axis=1, keepdims=True)


def take_blocks(grad, flags, owner_order, owners, replicas):
    rows, width = grad.shape
    cols = width // replicas
    pieces = rows // CHUNK

    def kernel(order_ref, flags_ref, grad_ref, out_ref, sems):
        me = lax.axis_index("dp")
        wanted = owners(me // 2, me % 2)

        def copies(k):
            start = pl.multiple_of(order_ref[wanted[k]] * cols, cols)
            return [
                pltpu.make_async_copy(
                    grad_ref.at[pl.ds(r * CHUNK, CHUNK), pl.ds(start, cols)],
                    out_ref.at[k, pl.ds(r * CHUNK, CHUNK)],
                    sems.at[k, r],
                )
                for r in range(pieces)
            ]

        started = [copies(k) for k in range(len(wanted))]
        for block in started:
            for copy in block:
                copy.start()
        kept = column((1 - flags_ref[...]).astype(jnp.float32))
        for k, block in enumerate(started):
            for r, copy in enumerate(block):
                copy.wait()
                at = pl.ds(r * CHUNK, CHUNK)
                out_ref[k, at] = out_ref[k, at] * kept[r * CHUNK:(r + 1) * CHUNK]

    count = len(owners(0, 0))
    return pl.pallas_call(
        kernel,
        out_shape=pltpu.VMEM((count, rows, cols), jnp.float32),
        in_specs=[in_smem(), in_vmem(), anywhere()],
        out_specs=in_vmem(),
        scratch_shapes=[pltpu.SemaphoreType.DMA((count, pieces))],
    )(owner_order, flags, grad)


def prefetch(step_count, master, moment_m, moment_v):
    def kernel(step_ref, w_ref, m_ref, v_ref, pw_ref, pm_ref, pv_ref, bias_ref, sems):
        pairs = ((m_ref, pm_ref), (v_ref, pv_ref), (w_ref, pw_ref))
        copies = [pltpu.make_async_copy(a, b, sems.at[i]) for i, (a, b) in enumerate(pairs)]
        for copy in copies:
            copy.start()
        lane = lax.broadcasted_iota(jnp.int32, (1, 128), 1)
        base = jnp.where(lane == 0, 0.9, 0.999).astype(jnp.float32)
        power = jnp.ones((1, 128), jnp.float32)
        steps = jnp.full((1, 128), step_ref[0], jnp.int32)
        for bit in range(31):
            power = jnp.where((steps >> bit) & 1 == 1, power * base, power)
            base = base * base
        bias_ref[...] = 1.0 - power
        for copy in copies:
            copy.wait()

    shape = master.shape
    return pl.pallas_call(
        kernel,
        out_shape=(
            pltpu.VMEM(shape, jnp.float32),
            pltpu.VMEM(shape, jnp.float32),
            pltpu.VMEM(shape, jnp.float32),
            pltpu.VMEM((1, 128), jnp.float32),
        ),
        in_specs=[in_smem(), anywhere(), anywhere(), anywhere()],
        out_specs=(in_vmem(), in_vmem(), in_vmem(), in_vmem()),
        scratch_shapes=[pltpu.SemaphoreType.DMA((3,))],
        name="prefetch",
    )(step_count, master, moment_m, moment_v)


def mean_and_squares(near, own_mate, arrived, count, flags, devices):
    rows, cols = near.shape

    def kernel(near_ref, mate_ref, count_ref, flags_ref, *refs):
        others, (grad_ref, row_ref) = refs[:-2], refs[-2:]
        scale = column(1.0 / jnp.maximum(count_ref[...], 1.0))
        squares = jnp.zeros((CHUNK, cols), jnp.float32)
        for r in range(rows // CHUNK):
            at = pl.ds(r * CHUNK, CHUNK)
            total = near_ref[at] + mate_ref[at]
            for other in others:
                total = total + other[at]
            part = total * scale[r * CHUNK:(r + 1) * CHUNK]
            grad_ref[at] = part
            squares = squares + part * part
        square = jnp.sum(jnp.sum(squares, axis=0, keepdims=True), axis=1, keepdims=True)
        dropped = jnp.sum(flags_ref[...].astype(jnp.float32), axis=1, keepdims=True)
        lane = lax.broadcasted_iota(jnp.int32, (1, 128), 1)
        row = jnp.where(lane == 0, square, jnp.where(lane == 1, dropped, 0.0))
        row_ref[...] = jnp.broadcast_to(row[None], (devices, 1, 128))

    return pl.pallas_call(
        kernel,
        out_shape=(pltpu.VMEM((rows, cols), jnp.float32), pltpu.VMEM((devices, 1, 128), jnp.float32)),
        in_specs=[in_vmem()] * (4 + len(arrived)),
        out_specs=(in_vmem(), in_vmem()),
        name="mean_and_squares",
    )(hold(near), hold(own_mate), count, flags, *map(hold, arrived))


def update(rows_of, grad, bias, weights, old_m, old_v, entries):
    rows, cols = grad.shape
    pieces = rows // CHUNK

    def kernel(rows_ref, grad_ref, bias_ref, w_ref, m_ref, v_ref, *refs):
        outs, dropped_ref, stages, sems = refs[:4], refs[4], refs[5:9], refs[9]
        totals = jnp.sum(rows_ref[...], axis=0)
        rms = jnp.sqrt(totals[:, 0:1] / entries)
        clip = jnp.minimum(1.0, 0.05 / (rms + 1e-06))
        m_scale = 1.0 / bias_ref[:, 0:1]
        v_scale = 1.0 / bias_ref[:, 1:2]
        started = []
        for r in range(pieces):
            at = pl.ds(r * CHUNK, CHUNK)
            g = grad_ref[at] * clip
            w = w_ref[at]
            new_m = 0.9 * m_ref[at] + 0.1 * g
            new_v = 0.999 * v_ref[at] + 0.001 * g * g
            direction = (new_m * m_scale) / (jnp.sqrt(new_v * v_scale) + 1e-08) + 0.1 * w
            values = (w - 0.001 * direction, new_m, new_v, direction)
            for i in range(4):
                stages[i][at] = values[i]
                copy = pltpu.make_async_copy(stages[i].at[at], outs[i].at[at], sems.at[i, r])
                copy.start()
                started.append(copy)
        dropped_ref[0] = jnp.sum(totals[:, 1:2]).astype(jnp.int32)
        for copy in started:
            copy.wait()

    shape = jax.ShapeDtypeStruct((rows, cols), jnp.float32)
    return pl.pallas_call(
        kernel,
        out_shape=(shape, shape, shape, shape, jax.ShapeDtypeStruct((1,), jnp.int32)),
        in_specs=[in_vmem()] * 6,
        out_specs=(anywhere(), anywhere(), anywhere(), anywhere(), in_smem()),
        scratch_shapes=[pltpu.VMEM((rows, cols), jnp.float32)] * 4 + [pltpu.SemaphoreType.DMA((4, pieces))],
        name="update",
    )(hold(rows_of), *map(hold, (grad, bias, weights, old_m, old_v)))


def body(grad_parts, drop_flags, owner_order, step_count, master, moment_m, moment_v):
    replicas = lax.axis_size("dp")
    chips = replicas // 2
    devices = lax.axis_size(ALL)
    flags = drop_flags[0, 0]
    local_grad = grad_parts[0, 0, 0]
    rows_here, width = local_grad.shape

    mate_pairs = [(j, j ^ 1) for j in range(replicas)]

    def along(step):
        return [(j, (j // 2 + step) % chips * 2 + j % 2) for j in range(replicas)]

    def far(chip, core):
        return [(chip + step) % chips * 2 + core for step in range(1, chips)]

    def near(chip, core):
        return [chip * 2 + core]

    def mates(owners):
        return lambda chip, core: owners(chip, 1 - core)

    def take(owners):
        return take_blocks(local_grad, flags, owner_order, owners, replicas)

    kept = (1 - flags).astype(jnp.float32)
    far_mate = take(mates(far))
    far_got = lax.ppermute(far_mate, "dp", mate_pairs)
    far_own = take(far)
    count = kept
    for step in range(1, chips):
        count = count + lax.ppermute(kept, "dp", along(step))
    far_sum = far_own + far_got
    arrived = []
    for step in range(1, chips):
        arrived.append(lax.ppermute(far_sum[step - 1], "dp", along(step)))
    near_mate = take(mates(near))[0]
    near_got = lax.ppermute(near_mate, "dp", mate_pairs)
    near_own = take(near)[0]
    weights, old_m, old_v, bias = prefetch(
        step_count.reshape(1), master[0, 0], moment_m[0, 0], moment_v[0, 0]
    )
    count = count + lax.ppermute(count, "dp", mate_pairs)
    grad, row = mean_and_squares(near_own, near_got, arrived, count, flags, devices)
    rows = lax.all_to_all(row, ALL, 0, 0, tiled=True)
    entries = rows_here * width * lax.axis_size("tensor") * lax.axis_size("pipe")
    new_master, new_m, new_v, direction, dropped = update(
        rows, grad, bias, weights, old_m, old_v, entries
    )
    return (
        new_master[None, None],
        new_m[None, None],
        new_v[None, None],
        direction[None, None],
        dropped.reshape(()),
    )


def solution(mesh):
    return jax.shard_map(
        body,
        mesh=mesh,
        in_specs=(
            P("dp", "pipe", "tensor", None, None),
            P("dp", "pipe", "tensor", None),
            P(),
            P(),
            P("pipe", "tensor", None, "dp"),
            P("pipe", "tensor", None, "dp"),
            P("pipe", "tensor", None, "dp"),
        ),
        out_specs=(
            P("pipe", "tensor", None, "dp"),
            P("pipe", "tensor", None, "dp"),
            P("pipe", "tensor", None, "dp"),
            P("pipe", "tensor", None, "dp"),
            P(),
        ),
        check_vma=False,
    )
```

```python
import jax
import jax.numpy as jnp
from jax import lax
from jax.experimental import pallas as pl
from jax.experimental.pallas import tpu as pltpu
from jax.sharding import PartitionSpec as P


ALL = ("dp", "tensor", "pipe")
VMEM = pltpu.MemorySpace.VMEM
SMEM = pltpu.MemorySpace.SMEM
CHUNK = 8


def in_vmem():
    return pl.BlockSpec(memory_space=VMEM)


def in_smem():
    return pl.BlockSpec(memory_space=SMEM)


def anywhere():
    return pl.BlockSpec(memory_space=pl.ANY)


def hold(x):
    return pltpu.with_memory_space_constraint(x, VMEM)


def column(row):
    n = row.shape[1]
    rows = lax.broadcasted_iota(jnp.int32, (n, n), 0)
    cols = lax.broadcasted_iota(jnp.int32, (n, n), 1)
    return jnp.sum(jnp.where(rows == cols, jnp.broadcast_to(row, (n, n)), 0.0), axis=1, keepdims=True)


def take_blocks(grad, flags, owner_order, owners, replicas):
    rows, width = grad.shape
    cols = width // replicas
    pieces = rows // CHUNK

    def kernel(order_ref, flags_ref, grad_ref, out_ref, flags_here, sems, flags_sem):
        flags_copy = pltpu.make_async_copy(flags_ref, flags_here, flags_sem)
        me = lax.axis_index("dp")
        wanted = owners(me // 2, me % 2)

        def copies(k):
            start = pl.multiple_of(order_ref[wanted[k]] * cols, cols)
            return [
                pltpu.make_async_copy(
                    grad_ref.at[pl.ds(r * CHUNK, CHUNK), pl.ds(start, cols)],
                    out_ref.at[k, pl.ds(r * CHUNK, CHUNK)],
                    sems.at[k, r],
                )
                for r in range(pieces)
            ]

        started = [copies(k) for k in range(len(wanted))]
        for block in started:
            for copy in block:
                copy.start()
        flags_copy.start()
        flags_copy.wait()
        kept = column((1 - flags_here[...]).astype(jnp.float32))
        for k, block in enumerate(started):
            for r, copy in enumerate(block):
                copy.wait()
                at = pl.ds(r * CHUNK, CHUNK)
                out_ref[k, at] = out_ref[k, at] * kept[r * CHUNK:(r + 1) * CHUNK]

    count = len(owners(0, 0))
    return pl.pallas_call(
        kernel,
        out_shape=pltpu.VMEM((count, rows, cols), jnp.float32),
        in_specs=[in_smem(), anywhere(), anywhere()],
        out_specs=in_vmem(),
        scratch_shapes=[
            pltpu.VMEM(flags.shape, flags.dtype),
            pltpu.SemaphoreType.DMA((count, pieces)),
            pltpu.SemaphoreType.DMA(()),
        ],
    )(owner_order, flags, grad)


def prefetch(step_count, master, moment_m, moment_v):
    def kernel(step_ref, w_ref, m_ref, v_ref, pw_ref, pm_ref, pv_ref, bias_ref, sems):
        pairs = ((m_ref, pm_ref), (v_ref, pv_ref), (w_ref, pw_ref))
        copies = [pltpu.make_async_copy(a, b, sems.at[i]) for i, (a, b) in enumerate(pairs)]
        for copy in copies:
            copy.start()
        lane = lax.broadcasted_iota(jnp.int32, (1, 128), 1)
        base = jnp.where(lane == 0, 0.9, 0.999).astype(jnp.float32)
        power = jnp.ones((1, 128), jnp.float32)
        steps = jnp.full((1, 128), step_ref[0], jnp.int32)
        for bit in range(31):
            power = jnp.where((steps >> bit) & 1 == 1, power * base, power)
            base = base * base
        bias_ref[...] = 1.0 - power
        for copy in copies:
            copy.wait()

    shape = master.shape
    return pl.pallas_call(
        kernel,
        out_shape=(
            pltpu.VMEM(shape, jnp.float32),
            pltpu.VMEM(shape, jnp.float32),
            pltpu.VMEM(shape, jnp.float32),
            pltpu.VMEM((1, 128), jnp.float32),
        ),
        in_specs=[in_smem(), anywhere(), anywhere(), anywhere()],
        out_specs=(in_vmem(), in_vmem(), in_vmem(), in_vmem()),
        scratch_shapes=[pltpu.SemaphoreType.DMA((3,))],
        name="prefetch",
    )(step_count, master, moment_m, moment_v)


def mean_and_squares(near, own_mate, arrived, count, kept, devices):
    rows, cols = near.shape

    def kernel(near_ref, mate_ref, count_ref, kept_ref, *refs):
        others, (grad_ref, row_ref) = refs[:-2], refs[-2:]
        scale = column(1.0 / jnp.maximum(count_ref[...], 1.0))
        squares = jnp.zeros((CHUNK, cols), jnp.float32)
        for r in range(rows // CHUNK):
            at = pl.ds(r * CHUNK, CHUNK)
            total = near_ref[at] + mate_ref[at]
            for other in others:
                total = total + other[at]
            part = total * scale[r * CHUNK:(r + 1) * CHUNK]
            grad_ref[at] = part
            squares = squares + part * part
        square = jnp.sum(jnp.sum(squares, axis=0, keepdims=True), axis=1, keepdims=True)
        dropped = jnp.sum(1.0 - kept_ref[...], axis=1, keepdims=True)
        lane = lax.broadcasted_iota(jnp.int32, (1, 128), 1)
        row = jnp.where(lane == 0, square, jnp.where(lane == 1, dropped, 0.0))
        row_ref[...] = jnp.broadcast_to(row[None], (devices, 1, 128))

    return pl.pallas_call(
        kernel,
        out_shape=(pltpu.VMEM((rows, cols), jnp.float32), pltpu.VMEM((devices, 1, 128), jnp.float32)),
        in_specs=[in_vmem()] * (4 + len(arrived)),
        out_specs=(in_vmem(), in_vmem()),
        name="mean_and_squares",
    )(*map(hold, (near, own_mate, count, kept, *arrived)))


def update(rows_of, grad, bias, weights, old_m, old_v, entries):
    rows, cols = grad.shape
    pieces = rows // CHUNK

    def kernel(rows_ref, grad_ref, bias_ref, w_ref, m_ref, v_ref, *refs):
        outs, dropped_ref, stages, sems, dropped_here, dropped_sem = refs[:4], refs[4], refs[5:9], *refs[9:]
        totals = jnp.sum(rows_ref[...], axis=0)
        dropped_here[...] = jnp.sum(totals[:, 1:2], axis=1, keepdims=True).astype(jnp.int32) + jnp.zeros((1, 128), jnp.int32)
        dropped_copy = pltpu.make_async_copy(dropped_here, dropped_ref, dropped_sem)
        dropped_copy.start()
        rms = jnp.sqrt(totals[:, 0:1] / entries)
        clip = jnp.minimum(1.0, 0.05 / (rms + 1e-06))
        m_scale = 1.0 / bias_ref[:, 0:1]
        v_scale = 1.0 / bias_ref[:, 1:2]
        started = []
        for r in range(pieces):
            at = pl.ds(r * CHUNK, CHUNK)
            g = grad_ref[at] * clip
            w = w_ref[at]
            new_m = 0.9 * m_ref[at] + 0.1 * g
            new_v = 0.999 * v_ref[at] + 0.001 * g * g
            direction = (new_m * m_scale) / (jnp.sqrt(new_v * v_scale) + 1e-08) + 0.1 * w
            values = (w - 0.001 * direction, new_m, new_v, direction)
            for i in range(4):
                stages[i][at] = values[i]
                copy = pltpu.make_async_copy(stages[i].at[at], outs[i].at[at], sems.at[i, r])
                copy.start()
                started.append(copy)
        dropped_copy.wait()
        for copy in started:
            copy.wait()

    shape = jax.ShapeDtypeStruct((rows, cols), jnp.float32)
    return pl.pallas_call(
        kernel,
        out_shape=(shape, shape, shape, shape, jax.ShapeDtypeStruct((1, 128), jnp.int32)),
        in_specs=[in_vmem()] * 6,
        out_specs=(anywhere(), anywhere(), anywhere(), anywhere(), anywhere()),
        scratch_shapes=[pltpu.VMEM((rows, cols), jnp.float32)] * 4 + [pltpu.SemaphoreType.DMA((4, pieces)), pltpu.VMEM((1, 128), jnp.int32), pltpu.SemaphoreType.DMA(())],
        name="update",
    )(hold(rows_of), *map(hold, (grad, bias, weights, old_m, old_v)))


def body(grad_parts, drop_flags, owner_order, step_count, master, moment_m, moment_v):
    replicas = lax.axis_size("dp")
    chips = replicas // 2
    devices = lax.axis_size(ALL)
    flags = drop_flags[0, 0]
    local_grad = grad_parts[0, 0, 0]
    rows_here, width = local_grad.shape

    mate_pairs = [(j, j ^ 1) for j in range(replicas)]

    def along(step):
        return [(j, (j // 2 + step) % chips * 2 + j % 2) for j in range(replicas)]

    def far(chip, core):
        return [(chip + step) % chips * 2 + core for step in range(1, chips)]

    def near(chip, core):
        return [chip * 2 + core]

    def mates(owners):
        return lambda chip, core: owners(chip, 1 - core)

    def take(owners):
        return take_blocks(local_grad, flags, owner_order, owners, replicas)

    kept = (1 - flags).astype(jnp.float32)
    far_mate = take(mates(far))
    far_got = lax.ppermute(far_mate, "dp", mate_pairs)
    far_own = take(far)
    count = kept
    for step in range(1, chips):
        count = count + lax.ppermute(kept, "dp", along(step))
    far_sum = far_own + far_got
    arrived = []
    for step in range(1, chips):
        arrived.append(lax.ppermute(far_sum[step - 1], "dp", along(step)))
    near_mate = take(mates(near))[0]
    near_got = lax.ppermute(near_mate, "dp", mate_pairs)
    near_own = take(near)[0]
    weights, old_m, old_v, bias = prefetch(
        step_count.reshape(1), master[0, 0], moment_m[0, 0], moment_v[0, 0]
    )
    count = count + lax.ppermute(count, "dp", mate_pairs)
    grad, row = mean_and_squares(near_own, near_got, arrived, count, kept, devices)
    rows = lax.all_to_all(row, ALL, 0, 0, tiled=True)
    entries = rows_here * width * lax.axis_size("tensor") * lax.axis_size("pipe")
    new_master, new_m, new_v, direction, dropped = update(
        rows, grad, bias, weights, old_m, old_v, entries
    )
    return (
        new_master[None, None],
        new_m[None, None],
        new_v[None, None],
        direction[None, None],
        dropped[0, 0],
    )


def solution(mesh):
    return jax.shard_map(
        body,
        mesh=mesh,
        in_specs=(
            P("dp", "pipe", "tensor", None, None),
            P("dp", "pipe", "tensor", None),
            P(),
            P(),
            P("pipe", "tensor", None, "dp"),
            P("pipe", "tensor", None, "dp"),
            P("pipe", "tensor", None, "dp"),
        ),
        out_specs=(
            P("pipe", "tensor", None, "dp"),
            P("pipe", "tensor", None, "dp"),
            P("pipe", "tensor", None, "dp"),
            P("pipe", "tensor", None, "dp"),
            P(),
        ),
        check_vma=False,
    )
```
